32 devices in a mesh: dp: 32 (over z, y, x, core), mp: 1.
Axes of the slice: x: 2, y: 2, z: 4, core: 2. Of those that a mesh axis runs over, the one named last changes fastest.
Arguments:
- gradients: bfloat16 [32, 512, 6144], P('dp', None, 'mp'), may hold values from -48 to 48
- weights: bfloat16 [512, 6144], P(None, 'mp'), may hold values from -3 to 3
- master: float32 [512, 6144], P('dp', 'mp'), may hold values from -6 to 6
- moment_one: float32 [512, 6144], P('dp', 'mp'), may hold values from -6 to 6
- moment_two: float32 [512, 6144], P('dp', 'mp'), may hold values from 0.25 to 4
- group_ids: int32 [512], replicated, may hold values from 0 to 15, never falling along the last dimension, each value on 1 to 64 neighbouring positions
Outputs:
- new_weights: bfloat16 [512, 6144], P(None, 'mp')
- new_master: float32 [512, 6144], P('dp', 'mp')
- new_first: float32 [512, 6144], P('dp', 'mp')
- new_second: float32 [512, 6144], P('dp', 'mp')
The draws below stay inside these ranges and needn't reach their ends.
Inputs may be any that keep to these rules, and one draw needn't show every extreme that they name: `group_ids`: group numbers never fall along the rows; each group has 1 to 64 rows and every group is present.
All inputs are finite; a program needn't handle non-finite values.
Results may differ from the reference program's by a relative error of at most 0.001.
The reference program's roundings to bfloat16 on the way count: a program that leaves them out, or rounds other values in their place, can miss the bound.
Values may be sent and summed in bfloat16 or wider, within the bound.
A program may use at most 64 MiB of HBM per device.

```python
import math
import jax
import jax.numpy as jnp
import numpy as np
from jax import lax

D = 6144
MOST = 64
ROWS_ALL = 512
GROUPS = 16
N_DP = 32


def raised(drawn, own_key, source, target, shards_of, factor):
    def block_of(dim):
        return (jnp.arange(drawn.shape[dim]) // (drawn.shape[dim] // shards_of)).reshape((-1,) + (1,) * (drawn.ndim - 1 - dim))

    first = jax.random.permutation(own_key, shards_of)[block_of(target)]
    other_side = (block_of(target) + shards_of // 2) % shards_of
    return jnp.where((block_of(source) == first) | (block_of(source) == other_side), factor * drawn, drawn)


def level_of(rng, extent, split, low, top_value):
    level = 1.0
    for axis_at, shards_of in split:
        draws = jax.random.uniform(jax.random.fold_in(jax.random.fold_in(rng, 6), axis_at), (shards_of,), jnp.float32, low / len(split), top_value / len(split))
        level = level * jnp.repeat(jnp.exp(draws), extent[axis_at] // shards_of).reshape((-1,) + (1,) * (len(extent) - 1 - axis_at))
    return level


def length_profile(amount, total, limit, slope):
    portions = [(1 << 20) // math.isqrt(grade ** slope) + 1 for grade in range(2, amount + 1)]
    rest, holding = total - limit - (amount - 1), [1] * (amount - 1)
    while rest > 0:
        candidates = [i for i in range(amount - 1) if holding[i] < limit]
        pool, budget = sum([portions[i] for i in candidates]), rest
        for i in candidates:
            more = min(limit - holding[i], max(1, budget * portions[i] // pool), rest)
            holding[i] = holding[i] + more
            rest = rest - more
    return np.array([limit] + holding)


def uneven(rng, number_of, total, most, lean):
    if number_of == 2:
        one = jax.random.randint(rng, (), max(1, total - most), min(most, total - 1) + 1)
        return jnp.stack([one, total - one])
    sizes = jnp.asarray(length_profile(number_of, total, most, lean), jnp.int32)
    pairs = (number_of - 1) // 2
    giver, sink = sizes[1:1 + 2 * pairs:2], sizes[2:2 + 2 * pairs:2]
    slack = jnp.minimum(giver - 1, most - sink)
    moved = jax.random.randint(jax.random.fold_in(rng, 1), (pairs,), 0, 1 << 20) % (slack + 1)
    sizes = sizes.at[1:1 + 2 * pairs:2].set(giver - moved).at[2:2 + 2 * pairs:2].set(sink + moved)
    return sizes[jax.random.permutation(jax.random.fold_in(rng, 2), number_of)]


def normal_values(stream_key, dims, deviation, most, shards=(), held_as=jnp.bfloat16):
    entries = deviation * jax.random.normal(stream_key, dims, jnp.float32)
    if shards:
        entries = entries * level_of(stream_key, dims, shards, -0.22, 0.18)
    return jnp.clip(entries, -most, most).astype(held_as)


def gaussian_with(stream_key, dims, scale, limit, pieces, heavy, kind=jnp.bfloat16):
    entries = scale * jax.random.normal(stream_key, dims, jnp.float32)
    if pieces:
        entries = entries * level_of(stream_key, dims, pieces, -0.22, 0.18)
    return jnp.clip(raised(entries, jax.random.fold_in(stream_key, 3), *heavy), -limit, limit).astype(kind)


def setup_inputs(seed: int = 0) -> dict:
    key_list = jax.random.split(jax.random.key(seed), 7)
    return {
        "gradients": gaussian_with(key_list[0], (N_DP, ROWS_ALL, D), 8.0, 48.0, ((0, 32),), (0, 1, 32, 2.75)),
        "weights": normal_values(key_list[1], (ROWS_ALL, D), 0.5, 3.0),
        "master": normal_values(key_list[2], (ROWS_ALL, D), 1.0, 6.0, ((0, 32),), jnp.float32),
        "moment_one": normal_values(key_list[3], (ROWS_ALL, D), 1.0, 6.0, ((0, 32),), jnp.float32),
        "moment_two": jnp.clip(jnp.exp(math.log(4.0) - 2.7725887 * jax.random.uniform(key_list[4], (ROWS_ALL, D), jnp.float32) ** level_of(key_list[4], (ROWS_ALL, D), ((0, 32),), -0.2, 0.2)), 0.25, 4.0),
        "group_ids": jnp.searchsorted(jnp.cumsum(uneven(key_list[5], GROUPS, ROWS_ALL, MOST, 0)), jnp.arange(ROWS_ALL), side="right").astype(jnp.int32),
    }


beta_one = 0.9
beta_two = 0.999
adam_eps = 1e-06
weight_decay = 0.01
learn_rate = 0.04
step_count = 100

def reference(gradients, weights, master, moment_one, moment_two, group_ids):
    grad_mean = lax.optimization_barrier(jnp.sum(gradients, axis=0, dtype=jnp.float32)) / N_DP
    new_first = beta_one * moment_one + (1.0 - beta_one) * grad_mean
    new_second = beta_two * moment_two + (1.0 - beta_two) * grad_mean * grad_mean
    correct_one = 1.0 - beta_one ** step_count
    correct_two = 1.0 - beta_two ** step_count
    update = new_first / correct_one / (jnp.sqrt(new_second / correct_two) + adam_eps) + weight_decay * master
    member = (group_ids[:, None] == jnp.arange(GROUPS, dtype=jnp.int32)[None, :]).astype(jnp.float32)
    weight_sq = jnp.dot(lax.optimization_barrier(jnp.sum(master * master, axis=1)), member, precision=lax.Precision.HIGHEST)
    update_sq = jnp.dot(lax.optimization_barrier(jnp.sum(update * update, axis=1)), member, precision=lax.Precision.HIGHEST)
    trust_ratio = jnp.sqrt(weight_sq / (update_sq + 1e-06))
    row_ratio = jnp.dot(member, trust_ratio, precision=lax.Precision.HIGHEST)
    step_size = learn_rate * row_ratio[:, None] * update
    new_master = master - step_size
    delta_bf = lax.optimization_barrier((-step_size).astype(jnp.bfloat16))
    new_weights = (weights.astype(jnp.float32) + delta_bf.astype(jnp.float32)).astype(jnp.bfloat16)
    return (new_weights, new_master, new_first, new_second)
```

```python
import functools

import jax
import jax.numpy as jnp
from jax import lax
from jax.experimental import pallas as pl
from jax.experimental.pallas import tpu as pltpu
from jax.sharding import PartitionSpec as P

beta_one = 0.9
beta_two = 0.999
adam_eps = 1e-06
weight_decay = 0.01
learn_rate = 0.04
step_count = 100

MESH = pl.DeviceIdType.MESH
F32, BF16 = jnp.float32, jnp.bfloat16
WIDTH = 512


def flipped(bit, flag):
    return bit + flag - 2 * bit * flag


def kernel(
    n, mp, width, ids_ref, grad_ref, w_ref, master_ref, m1_ref, m2_ref,
    out_ref, new_master_ref, new_first_ref, new_second_ref,
    mine, raw, acc, recvs, weights, held, update, member, tiles,
    mine_sem, w_sem, out_sem, rs_send, rs_recv, ag_send, ag_recv, t_send, t_recv,
):
    me = lax.axis_index("dp")
    bits = [(me // 2**i) % 2 for i in range(n)]
    replicas = 2**n
    rows, cols = master_ref.shape
    chunks = cols // width
    units = [list(range(j, min(j + 2, chunks))) for j in range(0, chunks, 2)]
    orders = []
    for k in range(chunks):
        order = list(range(n))
        if k % 2 and n > 2:
            order[1], order[2] = order[2], order[1]
        orders.append(order)

    def span(k):
        return pl.ds(k * width, width)

    def partner(flips):
        return sum(2**i * (1 - bits[i] if flips >> i & 1 else bits[i]) for i in range(n))

    low = min(n, 3)
    levels = [[{"dp": partner(f)} for f in range(1, 2**low)]]
    if n > low:
        levels.append([{"dp": partner(f << low)} for f in range(1, 2 ** (n - low))])
    if mp > 1:
        mine_mp = lax.axis_index("mp")
        places = mp.bit_length() - 1
        mp_bits = [(mine_mp // 2**i) % 2 for i in range(places)]
        levels.append([
            {"mp": sum(2**i * (1 - mp_bits[i] if f >> i & 1 else mp_bits[i]) for i in range(places))}
            for f in range(1, mp)
        ])

    w_copy = pltpu.make_async_copy(w_ref, weights, w_sem)
    mine_copies = [
        pltpu.make_async_copy(grad_ref.at[:, bits[0], :, span(k)], mine.at[k], mine_sem.at[k])
        for k in range(chunks)
    ]
    for copy in mine_copies:
        copy.start()

    barrier = pltpu.get_barrier_semaphore()
    greeted = [target for level in levels for target in level]
    for target in greeted:
        pl.semaphore_signal(barrier, inc=1, device_id=target, device_id_type=MESH)
    pl.semaphore_wait(barrier, len(greeted))

    started = []

    def send(src, dst, send_sem, recv_sem, target):
        copy = pltpu.make_async_remote_copy(
            src_ref=src, dst_ref=dst, send_sem=send_sem, recv_sem=recv_sem,
            device_id=target, device_id_type=MESH,
        )
        copy.start()
        started.append(copy)
        return copy

    rs = {}
    for k in range(chunks):
        rs[k, 0] = send(
            grad_ref.at[:, 1 - bits[0], :, span(k)], raw.at[k],
            rs_send.at[k, 0], rs_recv.at[k, 0], {"dp": partner(1)},
        )
    w_copy.start()

    lanes = member.shape[1]
    lane = lax.broadcasted_iota(jnp.int32, (rows, lanes), 1)
    row = lax.broadcasted_iota(jnp.int32, (rows, lanes), 0)
    own_ids = jnp.zeros((rows, lanes), jnp.int32)
    for r in range(rows):
        own_ids = jnp.where(row == r, ids_ref[me * rows + r], own_ids)
    member[...] = jnp.where(lane == own_ids, 1.0, 0.0).astype(F32)

    row_sums = {"w": jnp.zeros((rows, 1), F32), "u": jnp.zeros((rows, 1), F32)}
    correct_one = 1.0 - beta_one**step_count
    correct_two = 1.0 - beta_two**step_count

    def advance(k, s):
        order = orders[k]
        rs[k, s].wait_recv()
        if s == 0:
            mine_copies[k].wait()

            @pl.loop(0, 2 ** (n - 1))
            def _(d):
                rest = 0
                for i in range(n - 1):
                    b = order[n - 1 - i]
                    rest = rest + 2 ** (b - 1) * flipped(bits[b], (d // 2**i) % 2)
                acc[k, d] = mine[k, rest].astype(F32) + raw[k, rest].astype(F32)
            total = acc
        else:
            before = acc if s == 1 else recvs[s - 2]
            total = recvs[s - 1]

            @pl.loop(0, 2 ** (n - 1 - s))
            def _(d):
                total[k, d] = total[k, d] + before[k, d]
        if s < n - 1:
            half = 2 ** (n - 2 - s)
            rs[k, s + 1] = send(
                total.at[k, pl.ds(half, half)], recvs[s].at[k],
                rs_send.at[k, s + 1], rs_recv.at[k, s + 1],
                {"dp": partner(1 << order[s + 1])},
            )
            return
        grad_mean = total[k, 0] / replicas
        master = master_ref[:, span(k)]
        new_first = beta_one * m1_ref[:, span(k)] + (1.0 - beta_one) * grad_mean
        new_second = beta_two * m2_ref[:, span(k)] + (1.0 - beta_two) * grad_mean * grad_mean
        new_first_ref[:, span(k)] = new_first
        new_second_ref[:, span(k)] = new_second
        change = (
            new_first / correct_one / (jnp.sqrt(new_second / correct_two) + adam_eps)
            + weight_decay * master
        )
        update[:, span(k)] = change
        row_sums["w"] += jnp.sum(master * master, axis=1, keepdims=True)
        row_sums["u"] += jnp.sum(change * change, axis=1, keepdims=True)

    for t in range(len(units) + n - 1):
        for s in range(n):
            if 0 <= t - s < len(units):
                for k in units[t - s]:
                    advance(k, s)

    w_part = jnp.sum(member[...] * row_sums["w"], axis=0, keepdims=True)
    u_part = jnp.sum(member[...] * row_sums["u"], axis=0, keepdims=True)
    sub = lax.broadcasted_iota(jnp.int32, (8, lanes), 0)
    sums = jnp.where(sub == 0, w_part, u_part)
    at = 0
    for level, slots in zip(levels, tiles):
        slots[0] = sums
        copies = []
        for f, target in enumerate(level, 1):
            copies.append(send(slots.at[0], slots.at[f], t_send.at[at], t_recv.at[at], target))
            at += 1
        for f, copy in enumerate(copies, 1):
            copy.wait_recv()
            sums = sums + slots[f]
    trust = jnp.sqrt(sums[0:1] / (sums[1:2] + 1e-06))
    row_ratio = jnp.sum(member[...] * trust, axis=1, keepdims=True)
    scale = learn_rate * row_ratio

    ag = {}

    def gather(k, s):
        ag[k, s] = send(
            held.at[k, pl.ds(0, 2**s)], held.at[k, pl.ds(2**s, 2**s)],
            ag_send.at[k, s], ag_recv.at[k, s], {"dp": partner(1 << orders[k][n - 1 - s])},
        )

    for k in range(chunks):
        step = scale * update[:, span(k)]
        held[k, 0] = (-step).astype(BF16)
        gather(k, 0)
        new_master_ref[:, span(k)] = master_ref[:, span(k)] - step
    w_copy.wait()

    def apply(k, first, count):
        @pl.loop(first, first + count)
        def _(d):
            owner = 0
            for i in range(n):
                b = orders[k][n - 1 - i]
                owner = owner + 2**b * flipped(bits[b], (d // 2**i) % 2)
            weights[owner, :, span(k)] = (
                weights[owner, :, span(k)].astype(F32) + held[k, d].astype(F32)
            ).astype(BF16)

    outs = []
    for t in range(len(units) + n - 1):
        for s in range(n):
            if 0 <= t - s < len(units):
                for k in units[t - s]:
                    ag[k, s].wait_recv()
                    if s < n - 1:
                        gather(k, s + 1)
                    if s == n - 2:
                        apply(k, 0, 2 ** (n - 1))
                    elif s == n - 1:
                        apply(k, 2 ** (n - 1), 2 ** (n - 1))
                        copy = pltpu.make_async_copy(
                            weights.at[:, :, span(k)], out_ref.at[:, :, span(k)], out_sem.at[k]
                        )
                        copy.start()
                        outs.append(copy)
    for copy in started:
        copy.wait_send()
    for copy in outs:
        copy.wait()


def solution(mesh):
    replicas, mp = mesh.shape["dp"], mesh.shape["mp"]
    n = replicas.bit_length() - 1

    def on_device(gradients, weights, master, moment_one, moment_two, group_ids):
        rows_all, cols = weights.shape
        rows = master.shape[0]
        width = WIDTH if cols % WIDTH == 0 else 128
        chunks = cols // width
        groups = rows_all // 32
        lanes = -(-groups // 128) * 128
        low = min(n, 3)
        counts = [2**low] + ([2 ** (n - low)] if n > low else []) + ([mp] if mp > 1 else [])
        anywhere = pl.BlockSpec(memory_space=pl.ANY)
        vmem = pl.BlockSpec(memory_space=pltpu.VMEM)
        own = jax.ShapeDtypeStruct((rows, cols), F32)
        dma = pltpu.SemaphoreType.DMA
        tiles_n = sum(c - 1 for c in counts)
        new_weights, new_master, new_first, new_second = pl.pallas_call(
            functools.partial(kernel, n, mp, width),
            out_shape=(jax.ShapeDtypeStruct((replicas, rows, cols), BF16), own, own, own),
            in_specs=[pl.BlockSpec(memory_space=pltpu.SMEM), anywhere, anywhere, vmem, vmem, vmem],
            out_specs=(anywhere, vmem, vmem, vmem),
            scratch_shapes=[
                pltpu.VMEM((chunks, replicas // 2, rows, width), BF16),
                pltpu.VMEM((chunks, replicas // 2, rows, width), BF16),
                pltpu.VMEM((chunks, replicas // 2, rows, width), F32),
                [pltpu.VMEM((chunks, 2 ** (n - 1 - s), rows, width), F32) for s in range(1, n)],
                pltpu.VMEM((replicas, rows, cols), BF16),
                pltpu.VMEM((chunks, replicas, rows, width), BF16),
                pltpu.VMEM((rows, cols), F32),
                pltpu.VMEM((rows, lanes), F32),
                [pltpu.VMEM((c, 8, lanes), F32) for c in counts],
                dma((chunks,)),
                dma,
                dma((chunks,)),
                dma((chunks, n)),
                dma((chunks, n)),
                dma((chunks, n)),
                dma((chunks, n)),
                dma((tiles_n,)),
                dma((tiles_n,)),
            ],
            compiler_params=pltpu.CompilerParams(
                collective_id=0, has_side_effects=True, vmem_limit_bytes=56 * 2**20
            ),
        )(
            group_ids,
            gradients.reshape(replicas // 2, 2, rows, cols),
            weights.reshape(replicas, rows, cols),
            master, moment_one, moment_two,
        )
        return new_weights.reshape(rows_all, cols), new_master, new_first, new_second

    return jax.shard_map(
        on_device,
        mesh=mesh,
        in_specs=(P("dp", None, "mp"), P(None, "mp"), P("dp", "mp"), P("dp", "mp"), P("dp", "mp"), P()),
        out_specs=(P(None, "mp"), P("dp", "mp"), P("dp", "mp"), P("dp", "mp")),
        check_vma=False,
    )
```

```python
import functools

import jax
import jax.numpy as jnp
from jax import lax
from jax.experimental import pallas as pl
from jax.experimental.pallas import tpu as pltpu
from jax.sharding import PartitionSpec as P

beta_one = 0.9
beta_two = 0.999
adam_eps = 1e-06
weight_decay = 0.01
learn_rate = 0.04
step_count = 100

MESH = pl.DeviceIdType.MESH
F32, BF16 = jnp.float32, jnp.bfloat16
WIDTH = 512
SKEW = 2
AG_SKEW = 2
UNROLL = 4


def flipped(bit, flag):
    return bit + flag - 2 * bit * flag


def kernel(
    n, mp, width, ids_ref, grad_ref, w_ref, master_ref, m1_ref, m2_ref,
    out_ref, new_master_ref, new_first_ref, new_second_ref,
    mine, raw, acc, recvs, held, update, member, tiles,
    mine_sem, w_sem, rs_send, rs_recv, ag_send, ag_recv, t_send, t_recv,
):
    me = lax.axis_index("dp")
    bits = [(me // 2**i) % 2 for i in range(n)]
    replicas = 2**n
    rows, cols = master_ref.shape
    chunks = cols // width
    units = [list(range(j, min(j + 2, chunks))) for j in range(0, chunks, 2)]
    orders = []
    for k in range(chunks):
        order = list(range(n))
        if n > 3:
            order[1:4] = [2, 3, 1] if k % 2 else [1, 3, 2]
        orders.append(order)

    def span(k):
        return pl.ds(k * width, width)

    def partner(flips):
        return sum(2**i * (1 - bits[i] if flips >> i & 1 else bits[i]) for i in range(n))

    low = min(n, 3)
    levels = [[{"dp": partner(f)} for f in range(1, 2**low)]]
    if n > low:
        levels.append([{"dp": partner(f << low)} for f in range(1, 2 ** (n - low))])
    if mp > 1:
        mine_mp = lax.axis_index("mp")
        places = mp.bit_length() - 1
        mp_bits = [(mine_mp // 2**i) % 2 for i in range(places)]
        levels.append([
            {"mp": sum(2**i * (1 - mp_bits[i] if f >> i & 1 else mp_bits[i]) for i in range(places))}
            for f in range(1, mp)
        ])

    w_copy = pltpu.make_async_copy(w_ref, out_ref, w_sem)
    mine_copies = [
        pltpu.make_async_copy(grad_ref.at[:, bits[0], :, span(k)], mine.at[k], mine_sem.at[k])
        for k in range(chunks)
    ]
    for copy in mine_copies:
        copy.start()

    barrier = pltpu.get_barrier_semaphore()
    greeted = [target for level in levels for target in level]
    for target in greeted:
        pl.semaphore_signal(barrier, inc=1, device_id=target, device_id_type=MESH)
    pl.semaphore_wait(barrier, len(greeted))

    started = []

    def send(src, dst, send_sem, recv_sem, target):
        copy = pltpu.make_async_remote_copy(
            src_ref=src, dst_ref=dst, send_sem=send_sem, recv_sem=recv_sem,
            device_id=target, device_id_type=MESH,
        )
        copy.start()
        started.append(copy)
        return copy

    rs = {}
    for k in range(chunks):
        rs[k, 0] = send(
            grad_ref.at[:, 1 - bits[0], :, span(k)], raw.at[k],
            rs_send.at[k, 0], rs_recv.at[k, 0], {"dp": partner(1)},
        )
    w_copy.start()

    lanes = member.shape[1]
    lane = lax.broadcasted_iota(jnp.int32, (rows, lanes), 1)
    row = lax.broadcasted_iota(jnp.int32, (rows, lanes), 0)
    own_ids = jnp.zeros((rows, lanes), jnp.int32)
    for r in range(rows):
        own_ids = jnp.where(row == r, ids_ref[me * rows + r], own_ids)
    member[...] = jnp.where(lane == own_ids, 1.0, 0.0).astype(F32)

    row_sums = {"w": jnp.zeros((rows, 1), F32), "u": jnp.zeros((rows, 1), F32)}
    correct_one = 1.0 - beta_one**step_count
    correct_two = 1.0 - beta_two**step_count

    def advance(k, s):
        order = orders[k]
        rs[k, s].wait_recv()
        if s == 0:
            mine_copies[k].wait()

            @pl.loop(0, 2 ** (n - 1), unroll=min(UNROLL, 2 ** (n - 1)))
            def _(d):
                rest = 0
                for i in range(n - 1):
                    b = order[n - 1 - i]
                    rest = rest + 2 ** (b - 1) * flipped(bits[b], (d // 2**i) % 2)
                acc[k, d] = mine[k, rest].astype(F32) + raw[k, rest].astype(F32)
            total = acc
        else:
            before = acc if s == 1 else recvs[s - 2]
            total = recvs[s - 1]

            @pl.loop(0, 2 ** (n - 1 - s), unroll=min(UNROLL, 2 ** (n - 1 - s)))
            def _(d):
                total[k, d] = total[k, d] + before[k, d]
        if s < n - 1:
            half = 2 ** (n - 2 - s)
            rs[k, s + 1] = send(
                total.at[k, pl.ds(half, half)], recvs[s].at[k],
                rs_send.at[k, s + 1], rs_recv.at[k, s + 1],
                {"dp": partner(1 << order[s + 1])},
            )
            return
        grad_mean = total[k, 0] / replicas
        master = master_ref[:, span(k)]
        new_first = beta_one * m1_ref[:, span(k)] + (1.0 - beta_one) * grad_mean
        new_second = beta_two * m2_ref[:, span(k)] + (1.0 - beta_two) * grad_mean * grad_mean
        new_first_ref[:, span(k)] = new_first
        new_second_ref[:, span(k)] = new_second
        change = (
            new_first / correct_one / (jnp.sqrt(new_second / correct_two) + adam_eps)
            + weight_decay * master
        )
        update[:, span(k)] = change
        row_sums["w"] += jnp.sum(master * master, axis=1, keepdims=True)
        row_sums["u"] += jnp.sum(change * change, axis=1, keepdims=True)

    for t in range(len(units) + SKEW * (n - 1)):
        for s in range(n):
            if 0 <= t - SKEW * s < len(units):
                for k in units[t - SKEW * s]:
                    advance(k, s)

    w_part = jnp.sum(member[...] * row_sums["w"], axis=0, keepdims=True)
    u_part = jnp.sum(member[...] * row_sums["u"], axis=0, keepdims=True)
    sub = lax.broadcasted_iota(jnp.int32, (8, lanes), 0)
    sums = jnp.where(sub == 0, w_part, u_part)
    at = 0
    for level, slots in zip(levels, tiles):
        slots[0] = sums
        copies = []
        for f, target in enumerate(level, 1):
            copies.append(send(slots.at[0], slots.at[f], t_send.at[at], t_recv.at[at], target))
            at += 1
        for f, copy in enumerate(copies, 1):
            copy.wait_recv()
            sums = sums + slots[f]
    trust = jnp.sqrt(sums[0:1] / (sums[1:2] + 1e-06))
    row_ratio = jnp.sum(member[...] * trust, axis=1, keepdims=True)
    scale = learn_rate * row_ratio

    ag = {}

    def gather(k, s):
        ag[k, s] = send(
            held.at[k, pl.ds(0, 2**s)], held.at[k, pl.ds(2**s, 2**s)],
            ag_send.at[k, s], ag_recv.at[k, s], {"dp": partner(1 << orders[k][n - 1 - s])},
        )

    for k in range(chunks):
        step = scale * update[:, span(k)]
        held[k, 0] = (-step).astype(BF16)
        gather(k, 0)
        new_master_ref[:, span(k)] = master_ref[:, span(k)] - step
    w_copy.wait()

    def apply(k, first, count):
        @pl.loop(first, first + count, unroll=min(UNROLL, count))
        def _(d):
            owner = 0
            for i in range(n):
                b = orders[k][n - 1 - i]
                owner = owner + 2**b * flipped(bits[b], (d // 2**i) % 2)
            out_ref[owner, :, span(k)] = (
                out_ref[owner, :, span(k)].astype(F32) + held[k, d].astype(F32)
            ).astype(BF16)

    for t in range(len(units) + AG_SKEW * (n - 1)):
        for s in range(n):
            if 0 <= t - AG_SKEW * s < len(units):
                for k in units[t - AG_SKEW * s]:
                    ag[k, s].wait_recv()
                    if s < n - 1:
                        gather(k, s + 1)
                    if s == n - 2:
                        apply(k, 0, 2 ** (n - 1))
                    elif s == n - 1:
                        apply(k, 2 ** (n - 1), 2 ** (n - 1))
    for copy in started:
        copy.wait_send()


def solution(mesh):
    replicas, mp = mesh.shape["dp"], mesh.shape["mp"]
    n = replicas.bit_length() - 1

    def on_device(gradients, weights, master, moment_one, moment_two, group_ids):
        rows_all, cols = weights.shape
        rows = master.shape[0]
        width = WIDTH if cols % WIDTH == 0 else 128
        chunks = cols // width
        groups = rows_all // 32
        lanes = -(-groups // 128) * 128
        low = min(n, 3)
        counts = [2**low] + ([2 ** (n - low)] if n > low else []) + ([mp] if mp > 1 else [])
        anywhere = pl.BlockSpec(memory_space=pl.ANY)
        vmem = pl.BlockSpec(memory_space=pltpu.VMEM)
        own = pltpu.VMEM((rows, cols), F32)
        dma = pltpu.SemaphoreType.DMA
        tiles_n = sum(c - 1 for c in counts)
        new_weights, new_master, new_first, new_second = pl.pallas_call(
            functools.partial(kernel, n, mp, width),
            out_shape=(pltpu.VMEM((replicas, rows, cols), BF16), own, own, own),
            in_specs=[pl.BlockSpec(memory_space=pltpu.SMEM), anywhere, anywhere, vmem, vmem, vmem],
            out_specs=(vmem, vmem, vmem, vmem),
            scratch_shapes=[
                pltpu.VMEM((chunks, replicas // 2, rows, width), BF16),
                pltpu.VMEM((chunks, replicas // 2, rows, width), BF16),
                pltpu.VMEM((chunks, replicas // 2, rows, width), F32),
                [pltpu.VMEM((chunks, 2 ** (n - 1 - s), rows, width), F32) for s in range(1, n)],
                pltpu.VMEM((chunks, replicas, rows, width), BF16),
                pltpu.VMEM((rows, cols), F32),
                pltpu.VMEM((rows, lanes), F32),
                [pltpu.VMEM((c, 8, lanes), F32) for c in counts],
                dma((chunks,)),
                dma,
                dma((chunks, n)),
                dma((chunks, n)),
                dma((chunks, n)),
                dma((chunks, n)),
                dma((tiles_n,)),
                dma((tiles_n,)),
            ],
            compiler_params=pltpu.CompilerParams(
                collective_id=0, has_side_effects=True, vmem_limit_bytes=48 * 2**20
            ),
        )(
            group_ids,
            gradients.reshape(replicas // 2, 2, rows, cols),
            weights.reshape(replicas, rows, cols),
            master, moment_one, moment_two,
        )
        return new_weights.reshape(rows_all, cols), new_master, new_first, new_second

    return jax.shard_map(
        on_device,
        mesh=mesh,
        in_specs=(P("dp", None, "mp"), P(None, "mp"), P("dp", "mp"), P("dp", "mp"), P("dp", "mp"), P()),
        out_specs=(P(None, "mp"), P("dp", "mp"), P("dp", "mp"), P("dp", "mp")),
        check_vma=False,
    )
```
